32 devices in a mesh: grp: 2 (over x), seq: 4 (over y, core), tp: 4 (over z).
Axes of the slice: x: 2, y: 2, z: 4, core: 2. Of those that a mesh axis runs over, the one named last changes fastest.
Arguments:
- hidden: bfloat16 [2, 1024, 4096], P('grp', 'seq'), may hold values from -72 to 72
- w_query: bfloat16 [4096, 2048], P('seq', 'tp'), may hold values from -0.09375 to 0.09375
- w_key: bfloat16 [4096, 2048], P('seq', 'tp'), may hold values from -0.09375 to 0.09375
- w_value: bfloat16 [4096, 2048], P('seq', 'tp'), may hold values from -0.09375 to 0.09375
- prompt_len: int32 [256], replicated, may hold values from 1 to 1024
- page_table: int32 [256, 32], replicated, may hold values from 0 to 63, all different within a row
Outputs:
- attended: bfloat16 [2, 1024, 2048], P('grp', 'seq', 'tp')
The draws below stay inside these ranges and needn't reach their ends.
Inputs may be any that keep to these rules, and one draw needn't show every extreme that they name: `page_table`: every row lists 32 different pages; every page is listed by some row.
All inputs are finite; a program needn't handle non-finite values.
Results may differ from the reference program's by a relative error of at most 0.006.
The reference program's roundings to bfloat16 on the way count: a program that leaves them out, or rounds other values in their place, can miss the bound.
Values may be sent and summed in bfloat16 or wider, within the bound.
A program may use at most 128 MiB of HBM per device.

```python
import math
import jax
import jax.numpy as jnp
from jax import lax

D = 4096
HEADS = 16
HD = 128
PAGE = 16
STEPS = 4
ROWS = 256
PROMPT = 1024
PAGES = 64
CTXP = 32


def draw_hidden(key, part):
    base = jnp.clip(jax.random.normal(key, (2, PROMPT, D), jnp.float32), -6.0, 6.0)
    return base.astype(jnp.bfloat16)


def place_ends(values, stream_key, smallest, largest):
    longest = values.shape.index(max(values.shape))
    spots = []
    for shift in (0, 1):
        where = [jax.random.randint(jax.random.fold_in(stream_key, axis), (), 0, length) for axis, length in enumerate(values.shape)]
        where[longest] = (where[longest] + shift) % values.shape[longest]
        spots.append(tuple(where))
    return values.at[spots[0]].set(smallest).at[spots[1]].set(largest)


def block_levels(key, shape, cuts, least, high):
    factor_of = 1.0
    for dim, blocks in cuts:
        draws = jax.random.uniform(jax.random.fold_in(jax.random.fold_in(key, 6), dim), (blocks,), jnp.float32, least / len(cuts), high / len(cuts))
        factor_of = factor_of * jnp.repeat(jnp.exp(draws), shape[dim] // blocks).reshape((-1,) + (1,) * (len(shape) - 1 - dim))
    return factor_of


def different_ones(key, rows, amount, top, lift):
    ranking = jax.random.permutation(jax.random.fold_in(key, 1), amount)
    boost = ranking
    for power in range(3):
        boost = boost * boost // amount
    boost = boost * lift // amount
    chance = jax.random.randint(jax.random.fold_in(key, 2), (rows, amount), 0, 4096) + boost
    sure = jax.random.permutation(jax.random.fold_in(key, 3), rows)[jnp.arange(amount) % rows]
    chance = jnp.where(jnp.arange(rows)[:, None] == sure[None, :], 1 << 14, chance)
    score = chance * amount + jnp.arange(amount)
    return lax.top_k(score.astype(jnp.int32), top)[1].astype(jnp.int32)


def gaussian(stream_key, shape, deviation, reach, cuts=(), kind=jnp.bfloat16):
    loudness = block_levels(stream_key, shape, cuts, -0.22, 0.18) if cuts else 1.0
    values = jax.random.normal(stream_key, shape, jnp.float32) * deviation * loudness
    return jnp.minimum(jnp.maximum(values, -reach), reach).astype(kind)


def setup_inputs(seed: int = 0) -> dict:
    key_of = jax.random.split(jax.random.key(seed), 7)
    hidden = draw_hidden(jax.random.fold_in(key_of[6], 71), 0)
    w_query = gaussian(key_of[1], (D, HEADS * HD), D ** -0.5, 0.09375, ((0, 4), (1, 4)))
    w_key = gaussian(key_of[2], (D, HEADS * HD), D ** -0.5, 0.09375, ((0, 4), (1, 4)))
    w_value = gaussian(key_of[3], (D, HEADS * HD), D ** -0.5, 0.09375, ((0, 4), (1, 4)))
    prompt_len = place_ends(jax.random.randint(key_of[4], (ROWS,), 1, PROMPT + 1), jax.random.fold_in(key_of[4], 1), 1, PROMPT).astype(jnp.int32)
    page_table = different_ones(key_of[5], ROWS, PAGES, CTXP, 4096)
    return {"hidden": hidden, "w_query": w_query, "w_key": w_key, "w_value": w_value, "prompt_len": prompt_len, "page_table": page_table}


NEG = -1.0e30


def attend_head(query, keys, values, allowed):
    scores = jnp.dot(query, keys.T, preferred_element_type=jnp.float32) * (HD ** -0.5)
    scores = jnp.where(allowed, scores, NEG)
    top = jnp.max(scores, axis=1, keepdims=True)
    weights = jnp.where(allowed, jnp.exp(scores - top), 0.0)
    total = jnp.sum(weights, axis=1, keepdims=True)
    summed = jnp.dot(weights.astype(jnp.bfloat16), values, preferred_element_type=jnp.float32)
    return summed / total


def reference(hidden, w_query, w_key, w_value, prompt_len, page_table):
    flat_hidden = hidden.reshape(2 * PROMPT, D)

    def project(weight):
        out = jnp.dot(flat_hidden, weight, preferred_element_type=jnp.float32).astype(jnp.bfloat16)
        return out.reshape(2, PROMPT, HEADS, HD)

    query, keys, values = project(w_query), project(w_key), project(w_value)
    qblock = math.gcd(PROMPT, 512)

    def prefill_head(head):
        head_query, head_keys, head_values = head
        pieces = []
        for index in range(PROMPT // qblock):
            begin = index * qblock
            end = begin + qblock
            query_pos = jnp.arange(begin, end).astype(jnp.int32)
            key_pos = jnp.arange(end).astype(jnp.int32)
            allowed = key_pos[None, :] <= query_pos[:, None]
            pieces.append(attend_head(head_query[begin:end], head_keys[:end], head_values[:end], allowed))
        return jnp.concatenate(pieces, axis=0).astype(jnp.bfloat16)

    prefill = lax.map(prefill_head, (query[0].transpose(1, 0, 2), keys[0].transpose(1, 0, 2), values[0].transpose(1, 0, 2)))
    prefill = prefill.transpose(1, 0, 2).reshape(PROMPT, HEADS * HD)

    rblock = math.gcd(ROWS, 8)
    offsets = jnp.arange(PAGE).astype(jnp.int32)
    causal_steps = jnp.arange(STEPS)[None, :] <= jnp.arange(STEPS)[:, None]

    def decode_block(index):
        first_row = index * rblock
        tables = lax.dynamic_slice_in_dim(page_table, first_row, rblock, 0)
        lengths = lax.dynamic_slice_in_dim(prompt_len, first_row, rblock, 0)
        key_pos = (tables[:, :, None] * PAGE + offsets[None, None, :]).reshape(rblock, CTXP * PAGE)
        context_allowed = key_pos < lengths[:, None]
        context_keys = keys[0][key_pos]
        context_values = values[0][key_pos]
        first_pos = first_row * STEPS
        block_query = lax.dynamic_slice_in_dim(query[1], first_pos, rblock * STEPS, 0).reshape(rblock, STEPS, HEADS, HD)
        own_keys = lax.dynamic_slice_in_dim(keys[1], first_pos, rblock * STEPS, 0).reshape(rblock, STEPS, HEADS, HD)
        own_values = lax.dynamic_slice_in_dim(values[1], first_pos, rblock * STEPS, 0).reshape(rblock, STEPS, HEADS, HD)
        all_keys = jnp.concatenate([context_keys, own_keys], axis=1)
        all_values = jnp.concatenate([context_values, own_values], axis=1)
        allowed = jnp.concatenate([
            jnp.broadcast_to(context_allowed[:, None, :], (rblock, STEPS, CTXP * PAGE)),
            jnp.broadcast_to(causal_steps[None], (rblock, STEPS, STEPS))], axis=2)
        scores = jnp.einsum("rshd,rkhd->rhsk", block_query.astype(jnp.float32), all_keys.astype(jnp.float32)) * (HD ** -0.5)
        scores = jnp.where(allowed[:, None], scores, NEG)
        top = jnp.max(scores, axis=3, keepdims=True)
        weights = jnp.where(allowed[:, None], jnp.exp(scores - top), 0.0)
        total = jnp.sum(weights, axis=3)
        summed = jnp.einsum("rhsk,rkhd->rshd", weights.astype(jnp.bfloat16).astype(jnp.float32), all_values.astype(jnp.float32))
        result = summed / total.transpose(0, 2, 1)[:, :, :, None]
        return result.reshape(rblock * STEPS, HEADS * HD).astype(jnp.bfloat16)

    decode = lax.map(decode_block, jnp.arange(ROWS // rblock).astype(jnp.int32)).reshape(PROMPT, HEADS * HD)
    return jnp.stack([prefill, decode])
```

```python
import math

import jax
import jax.numpy as jnp
from jax import lax
from jax.experimental import pallas as pl
from jax.experimental.pallas import tpu as pltpu
from jax.sharding import PartitionSpec as P

HD = 128
PAGE = 16
STEPS = 4


NEG = -1e30


def from_behind(value, axis, steps):
    count = lax.axis_size(axis)
    first, last = (max(0, -steps), min(count, count - steps))
    return lax.ppermute(value, axis, [(source, source + steps) for source in range(first, last)])


def partial_attention(query, keys, values, allowed):
    rows = query.shape[0]
    heads = query.shape[1] // HD
    query_heads = query.reshape(rows, heads, HD)
    key_heads = keys.reshape(keys.shape[0], heads, HD)
    value_heads = values.reshape(values.shape[0], heads, HD)
    scores = jnp.einsum(
        "rhd,shd->hrs", query_heads, key_heads, preferred_element_type=jnp.float32
    ) * HD ** (-0.5)
    scores = jnp.where(allowed[None], scores, NEG)
    top = jnp.max(scores, axis=2)
    weights = jnp.where(allowed[None], jnp.exp(scores - top[:, :, None]), 0.0)
    total = jnp.sum(weights, axis=2)
    summed = jnp.einsum(
        "hrs,shd->rhd",
        weights.astype(jnp.bfloat16),
        value_heads,
        preferred_element_type=jnp.float32,
    )
    return (top, total, summed.reshape(rows, heads * HD))


def rescale(summed, factor):
    rows = summed.shape[0]
    heads = factor.shape[0]
    return (summed.reshape(rows, heads, HD) * factor.T[:, :, None]).reshape(rows, heads * HD)


def combine(first, second):
    top = jnp.maximum(first[0], second[0])
    early = jnp.exp(first[0] - top)
    later = jnp.exp(second[0] - top)
    return (
        top,
        first[1] * early + second[1] * later,
        rescale(first[2], early) + rescale(second[2], later),
    )


def finish(state):
    return rescale(state[2], 1.0 / state[1]).astype(jnp.bfloat16)


def row_mask(tables, lengths, key_pos):
    pages = key_pos // PAGE
    member = jnp.any(tables[:, :, None] == pages[None, None, :], axis=1)
    allowed = member & (key_pos[None, :] < lengths[:, None])
    return jnp.repeat(allowed, STEPS, axis=0)


def blocked(carry, keys, values, query, mask_of):
    count = keys.shape[0]
    block = math.gcd(count, 512)

    def one_block(state, offset):
        piece_keys = lax.dynamic_slice_in_dim(keys, offset, block, 0)
        piece_values = lax.dynamic_slice_in_dim(values, offset, block, 0)
        key_pos = offset + jnp.arange(block)
        return (
            combine(state, partial_attention(query, piece_keys, piece_values, mask_of(key_pos))),
            None,
        )

    offsets = jnp.arange(count // block) * block
    state, unused = lax.scan(one_block, carry, offsets)
    return state


def on_device(hidden, w_query, w_key, w_value, prompt_len, page_table):
    local = hidden[0]
    rows = local.shape[0]
    width = w_query.shape[1]
    heads = width // HD
    seq_index = lax.axis_index("seq")
    is_prompt = lax.axis_index("grp") == 0
    empty = jnp.zeros((rows, width), jnp.float32)
    piece = (
        lax.all_gather(w_query, "seq", axis=0, tiled=True),
        lax.all_gather(w_key, "seq", axis=0, tiled=True),
        lax.all_gather(w_value, "seq", axis=0, tiled=True),
    )
    projected = tuple(
        (jnp.dot(local, weight, preferred_element_type=jnp.float32) for weight in piece)
    )
    query, keys, values = [item.astype(jnp.bfloat16) for item in projected]
    positions = seq_index * rows + jnp.arange(rows)
    start_state = (
        jnp.full((heads, rows), NEG, jnp.float32),
        jnp.zeros((heads, rows), jnp.float32),
        empty,
    )
    given_keys, given_values = from_behind((keys, values), "grp", 1)
    cache_keys = jnp.where(is_prompt, keys, given_keys)
    cache_values = jnp.where(is_prompt, values, given_values)
    row_count = rows // STEPS
    own_tables = lax.dynamic_slice_in_dim(page_table, seq_index * row_count, row_count, 0)
    own_lengths = lax.dynamic_slice_in_dim(prompt_len, seq_index * row_count, row_count, 0)

    def mask_of(key_pos):
        causal = key_pos[None, :] <= positions[:, None]
        listed = row_mask(own_tables, own_lengths, key_pos)
        return jnp.where(is_prompt, causal, listed)

    piece = (
        lax.all_gather(cache_keys, "seq", axis=0, tiled=True),
        lax.all_gather(cache_values, "seq", axis=0, tiled=True),
    )
    state = blocked(start_state, piece[0], piece[1], query, mask_of)
    frame_row = positions // STEPS
    own_rows = (frame_row[:, None] == frame_row[None, :]) & (
        positions[None, :] <= positions[:, None]
    )
    fresh = partial_attention(query, keys, values, own_rows)
    prefill_out = finish(state)
    decode_out = finish(combine(state, fresh))
    return jnp.where(is_prompt, prefill_out, decode_out)[None]


QUERY, KEY, VALUE = 0, 1, 2
ORDER = (KEY, VALUE, QUERY)
SUBS = 2
PARTS = 2


def fused_kernel(
    hidden, w_query, w_key, w_value, lengths, tables, out,
    hbuf, near, far, acc, qbuf, fresh, cache, bias, osend, orecv,
    y_send, y_recv, x_send, x_recv, d_send, d_recv, local_sem,
    kx_send, kx_recv, ky_send, ky_recv, o_send, o_recv,
):
    weights = {QUERY: w_query, KEY: w_key, VALUE: w_value}
    rows = hidden.shape[1]
    depth = w_query.shape[0]
    half = w_query.shape[1] // 2
    heads = half // HD
    chip_rows = 2 * rows
    grp = lax.axis_index("grp")
    seq = lax.axis_index("seq")
    y = seq // 2
    core = seq % 2
    partner = {"seq": 2 * y + 1 - core}
    across = [{"seq": 2 * (1 - y) + core}, {"seq": 2 * (1 - y) + 1 - core}]
    beside = {"grp": 1 - grp}
    core_of = [core, 1 - core]
    piece = depth // 2 // SUBS

    barrier = pltpu.get_barrier_semaphore()
    for other in (partner, across[0], across[1], beside):
        pl.semaphore_signal(barrier, inc=1, device_id=other, device_id_type=pl.DeviceIdType.MESH)
    pl.semaphore_wait(barrier, 4)

    def remote(src, dst, send, recv, to):
        return pltpu.make_async_remote_copy(
            src_ref=src, dst_ref=dst, send_sem=send, recv_sem=recv,
            device_id=to, device_id_type=pl.DeviceIdType.MESH,
        )

    def columns(which):
        return pl.ds(pl.multiple_of(core_of[which] * half, half), half)

    steps = [(m, sub, rel) for m in ORDER for sub in range(SUBS) for rel in range(2)]

    def slot(m, rel, way, sub):
        return ((m * 2 + rel) * 2 + way) * SUBS + sub

    def weight_copy(m, sub, rel):
        first = pl.multiple_of(grp * (depth // 2) + sub * piece, piece)
        at = slot(m, rel, 0, sub)
        return remote(
            weights[m].at[pl.ds(first, piece), columns(rel)],
            far.at[at], y_send.at[at], y_recv.at[at], across[rel],
        )

    def forward_copy(m, sub, rel):
        source, target = slot(m, rel, 0, sub), slot(m, rel, 1, sub)
        return remote(far.at[source], far.at[target], x_send.at[target], x_recv.at[target], beside)

    sent = []
    for step in steps:
        copy = weight_copy(*step)
        copy.start()
        sent.append(copy)
    my_rows = pl.ds(pl.multiple_of(core * rows, rows), rows)
    hidden_swap = remote(hidden.at[0], hbuf.at[my_rows], d_send.at[3], d_recv.at[3], partner)
    hidden_swap.start()
    swaps = {
        m: remote(weights[m].at[:, columns(1)], near.at[2 * m + 1], d_send.at[m], d_recv.at[m], partner)
        for m in ORDER
    }
    keeps = {
        m: pltpu.make_async_copy(weights[m].at[:, columns(0)], near.at[2 * m], local_sem.at[m])
        for m in ORDER
    }
    hidden_keep = pltpu.make_async_copy(hidden.at[0], hbuf.at[my_rows], local_sem.at[3])
    hidden_keep.start()
    for m in ORDER:
        keeps[m].start()
        swaps[m].start()
    sent += [hidden_swap] + [swaps[m] for m in ORDER]

    decode_rows = chip_rows // STEPS
    all_rows = lengths.shape[1]
    pages = 2 * chip_rows // PAGE
    own_table = tables[pl.ds(pl.multiple_of(y * decode_rows, decode_rows), decode_rows), :]
    page_lane = lax.broadcasted_iota(jnp.int32, (decode_rows, pages), 1)
    member = own_table[:, 0:1] == page_lane
    for listed in range(1, own_table.shape[1]):
        member = member | (own_table[:, listed : listed + 1] == page_lane)
    member = jnp.where(member, 1.0, 0.0).astype(jnp.bfloat16)
    pick = (
        lax.broadcasted_iota(jnp.int32, (decode_rows, all_rows), 1)
        == lax.broadcasted_iota(jnp.int32, (decode_rows, all_rows), 0) + y * decode_rows
    )
    own_length = jnp.sum(jnp.where(pick, lengths[...], 0), axis=1, keepdims=True)
    step_bits = STEPS.bit_length() - 1
    page_bits = PAGE.bit_length() - 1
    spread = (
        lax.shift_right_logical(lax.broadcasted_iota(jnp.int32, (chip_rows, decode_rows), 0), step_bits)
        == lax.broadcasted_iota(jnp.int32, (chip_rows, decode_rows), 1)
    )
    spread = jnp.where(spread, 1.0, 0.0).astype(jnp.bfloat16)
    prompt_one = jnp.where(grp == 0, 1, 0)
    for side in range(2):
        base = (y if side == 0 else 1 - y) * chip_rows
        key_page = lax.shift_right_logical(
            lax.broadcasted_iota(jnp.int32, (pages, chip_rows), 1) + base, page_bits
        )
        unfold = lax.broadcasted_iota(jnp.int32, (pages, chip_rows), 0) == key_page
        unfold = jnp.where(unfold, 1.0, 0.0).astype(jnp.bfloat16)
        seen = jnp.dot(member, unfold, preferred_element_type=jnp.float32)
        key_pos = lax.broadcasted_iota(jnp.int32, (decode_rows, chip_rows), 1) + base
        seen = jnp.where(key_pos < own_length, seen, 0.0).astype(jnp.bfloat16)
        listed = jnp.dot(spread, seen, preferred_element_type=jnp.float32)
        causal = (
            lax.broadcasted_iota(jnp.int32, (chip_rows, chip_rows), 1) + base
            <= lax.broadcasted_iota(jnp.int32, (chip_rows, chip_rows), 0) + y * chip_rows
        )
        causal = jnp.where(causal, 1.0, 0.0)
        allowed = jnp.where(prompt_one == 1, causal, listed)
        bias[:, side * chip_rows : (side + 1) * chip_rows] = jnp.where(allowed > 0.5, 0.0, NEG)

    def add(m, weight, first, count, fresh_start=False):
        left = hbuf[:, pl.ds(pl.multiple_of(first, count), count)]
        product = jnp.dot(left, weight, preferred_element_type=jnp.float32)
        if fresh_start:
            acc[m] = product
        else:
            acc[m] += product

    hidden_keep.wait()
    hidden_swap.wait_recv()
    for m in ORDER:
        keeps[m].wait()
        add(m, near[2 * m], (2 * y + core) * depth, depth, True)
        swaps[m].wait_recv()
        add(m, near[2 * m + 1], (2 * y + 1 - core) * depth, depth)

    def from_across(m, sub, rel, way):
        owner = grp if way == 0 else 1 - grp
        first = (2 * (1 - y) + core_of[rel]) * depth + owner * (depth // 2) + sub * piece
        add(m, far[slot(m, rel, way, sub)], first, piece)

    def take_y(step):
        weight_copy(*step).wait_recv()
        copy = forward_copy(*step)
        copy.start()
        sent.append(copy)
        from_across(*step, 0)

    def take_x(step):
        forward_copy(*step).wait_recv()
        from_across(*step, 1)

    kv_steps = [step for step in steps if step[0] != QUERY]
    q_steps = [step for step in steps if step[0] == QUERY]
    lag = 2
    for index, step in enumerate(kv_steps):
        take_y(step)
        if index >= lag:
            take_x(kv_steps[index - lag])
    for step in kv_steps[-lag:]:
        take_x(step)

    kv_pieces = [(kind, part) for kind in range(2) for part in range(PARTS)]
    part_rows = chip_rows // PARTS

    def piece_of(ref, at, part):
        return ref.at[at, pl.ds(part * part_rows, part_rows)]

    def kx_copy(kind, part):
        at = kind * PARTS + part
        return remote(
            piece_of(fresh, kind, part), piece_of(cache, kind, part), kx_send.at[at], kx_recv.at[at], beside
        )

    def ky_copy(kind, part, source):
        at = kind * PARTS + part
        return remote(
            piece_of(source, kind, part), piece_of(cache, 2 + kind, part),
            ky_send.at[at], ky_recv.at[at], across[0],
        )

    fresh[0] = acc[KEY].astype(jnp.bfloat16)
    fresh[1] = acc[VALUE].astype(jnp.bfloat16)

    @pl.when(grp == 0)
    def _():
        for kind, part in kv_pieces:
            kx_copy(kind, part).start()
            ky_copy(kind, part, fresh).start()
        cache[0] = acc[KEY].astype(jnp.bfloat16)
        cache[1] = acc[VALUE].astype(jnp.bfloat16)

    for step in q_steps:
        take_y(step)

    @pl.when(grp != 0)
    def _():
        for kind, part in kv_pieces:
            kx_copy(kind, part).wait_recv()
            ky_copy(kind, part, cache).start()

    for step in q_steps:
        take_x(step)
    qbuf[...] = acc[QUERY].astype(jnp.bfloat16)
    for kind, part in kv_pieces:
        ky_copy(kind, part, cache).wait_recv()

    block = min(rows, 128)
    contract_last = (((1,), (1,)), ((), ()))
    fresh_row = lax.broadcasted_iota(jnp.int32, (block, block), 0)
    fresh_col = lax.broadcasted_iota(jnp.int32, (block, block), 1)
    same = (
        lax.shift_right_logical(fresh_row, step_bits) == lax.shift_right_logical(fresh_col, step_bits)
    ) & (fresh_col <= fresh_row)
    fresh_bias = jnp.where(jnp.where(same, 1 - prompt_one, 0) == 1, 0.0, NEG)
    scale = HD ** (-0.5)

    def attend(first, head):
        span = pl.ds(pl.multiple_of(first, block), block)
        lanes = slice(head * HD, (head + 1) * HD)
        query = qbuf[span, lanes]

        def scored(keys, mask):
            return lax.dot_general(
                query, keys, contract_last, preferred_element_type=jnp.float32
            ) * scale + mask

        scores = [
            scored(cache[0, :, lanes], bias[span, 0:chip_rows]),
            scored(cache[2, :, lanes], bias[span, chip_rows : 2 * chip_rows]),
            scored(fresh[0, span, lanes], fresh_bias),
        ]
        values = [cache[1, :, lanes], cache[3, :, lanes], fresh[1, span, lanes]]
        top = jnp.maximum(
            jnp.maximum(
                jnp.max(scores[0], axis=1, keepdims=True), jnp.max(scores[1], axis=1, keepdims=True)
            ),
            jnp.max(scores[2], axis=1, keepdims=True),
        )
        total = jnp.zeros((block, 1), jnp.float32)
        summed = jnp.zeros((block, HD), jnp.float32)
        for score, value in zip(scores, values):
            weight = jnp.exp(score - top)
            total += jnp.sum(weight, axis=1, keepdims=True)
            summed += jnp.dot(weight.astype(jnp.bfloat16), value, preferred_element_type=jnp.float32)
        return (summed / total).astype(jnp.bfloat16)

    for at in range(rows // block):
        for head in range(heads):
            osend[at * block : (at + 1) * block, head * HD : (head + 1) * HD] = attend(
                (1 - core) * rows + at * block, head
            )
    swap_out = remote(osend, orecv, o_send, o_recv, partner)
    swap_out.start()
    for at in range(rows // block):
        for head in range(heads):
            out[at * block : (at + 1) * block, pl.ds(pl.multiple_of(core * half + head * HD, HD), HD)] = attend(
                core * rows + at * block, head
            )
    swap_out.wait()
    out[:, columns(1)] = orecv[...]

    for copy in sent:
        copy.wait_send()

    @pl.when(grp == 0)
    def _():
        for kind, part in kv_pieces:
            kx_copy(kind, part).wait_send()
            ky_copy(kind, part, fresh).wait_send()

    @pl.when(grp != 0)
    def _():
        for kind, part in kv_pieces:
            ky_copy(kind, part, cache).wait_send()


def fused(hidden, w_query, w_key, w_value, prompt_len, page_table):
    rows, model = hidden.shape[1:]
    depth, width = w_query.shape
    half = width // 2
    chip_rows = 2 * rows
    slots = 3 * 2 * 2 * SUBS
    dma = pltpu.SemaphoreType.DMA
    anywhere = pl.BlockSpec(memory_space=pl.ANY)
    vmem = pl.BlockSpec(memory_space=pltpu.VMEM)
    result = pl.pallas_call(
        fused_kernel,
        out_shape=jax.ShapeDtypeStruct((rows, width), jnp.bfloat16),
        in_specs=[anywhere] * 4 + [vmem] * 2,
        out_specs=vmem,
        scratch_shapes=[
            pltpu.VMEM((chip_rows, model), jnp.bfloat16),
            pltpu.VMEM((6, depth, half), jnp.bfloat16),
            pltpu.VMEM((slots, depth // 2 // SUBS, half), jnp.bfloat16),
            pltpu.VMEM((3, chip_rows, half), jnp.float32),
            pltpu.VMEM((chip_rows, half), jnp.bfloat16),
            pltpu.VMEM((2, chip_rows, half), jnp.bfloat16),
            pltpu.VMEM((4, chip_rows, half), jnp.bfloat16),
            pltpu.VMEM((chip_rows, 2 * chip_rows), jnp.float32),
            pltpu.VMEM((rows, half), jnp.bfloat16),
            pltpu.VMEM((rows, half), jnp.bfloat16),
            dma((slots,)), dma((slots,)), dma((slots,)), dma((slots,)),
            dma((4,)), dma((4,)), dma((4,)),
            dma((2 * PARTS,)), dma((2 * PARTS,)), dma((2 * PARTS,)), dma((2 * PARTS,)),
            dma, dma,
        ],
        compiler_params=pltpu.CompilerParams(
            collective_id=0, has_side_effects=True, vmem_limit_bytes=48 * 1024 * 1024
        ),
    )(hidden, w_query, w_key, w_value, prompt_len.reshape(1, -1), page_table)
    return result[None]


def solution(mesh):
    paired = mesh.shape["grp"] == 2 and mesh.shape["seq"] == 4
    return jax.shard_map(
        fused if paired else on_device,
        mesh=mesh,
        in_specs=(P("grp", "seq", None), P("seq", "tp"), P("seq", "tp"), P("seq", "tp"), P(), P()),
        out_specs=P("grp", "seq", "tp"),
        check_vma=False,
    )
```

```python
import math

import jax
import jax.numpy as jnp
from jax import lax
from jax.experimental import pallas as pl
from jax.experimental.pallas import tpu as pltpu
from jax.sharding import PartitionSpec as P

HD = 128
PAGE = 16
STEPS = 4


NEG = -1e30


def from_behind(value, axis, steps):
    count = lax.axis_size(axis)
    first, last = (max(0, -steps), min(count, count - steps))
    return lax.ppermute(value, axis, [(source, source + steps) for source in range(first, last)])


def partial_attention(query, keys, values, allowed):
    rows = query.shape[0]
    heads = query.shape[1] // HD
    query_heads = query.reshape(rows, heads, HD)
    key_heads = keys.reshape(keys.shape[0], heads, HD)
    value_heads = values.reshape(values.shape[0], heads, HD)
    scores = jnp.einsum(
        "rhd,shd->hrs", query_heads, key_heads, preferred_element_type=jnp.float32
    ) * HD ** (-0.5)
    scores = jnp.where(allowed[None], scores, NEG)
    top = jnp.max(scores, axis=2)
    weights = jnp.where(allowed[None], jnp.exp(scores - top[:, :, None]), 0.0)
    total = jnp.sum(weights, axis=2)
    summed = jnp.einsum(
        "hrs,shd->rhd",
        weights.astype(jnp.bfloat16),
        value_heads,
        preferred_element_type=jnp.float32,
    )
    return (top, total, summed.reshape(rows, heads * HD))


def rescale(summed, factor):
    rows = summed.shape[0]
    heads = factor.shape[0]
    return (summed.reshape(rows, heads, HD) * factor.T[:, :, None]).reshape(rows, heads * HD)


def combine(first, second):
    top = jnp.maximum(first[0], second[0])
    early = jnp.exp(first[0] - top)
    later = jnp.exp(second[0] - top)
    return (
        top,
        first[1] * early + second[1] * later,
        rescale(first[2], early) + rescale(second[2], later),
    )


def finish(state):
    return rescale(state[2], 1.0 / state[1]).astype(jnp.bfloat16)


def row_mask(tables, lengths, key_pos):
    pages = key_pos // PAGE
    member = jnp.any(tables[:, :, None] == pages[None, None, :], axis=1)
    allowed = member & (key_pos[None, :] < lengths[:, None])
    return jnp.repeat(allowed, STEPS, axis=0)


def blocked(carry, keys, values, query, mask_of):
    count = keys.shape[0]
    block = math.gcd(count, 512)

    def one_block(state, offset):
        piece_keys = lax.dynamic_slice_in_dim(keys, offset, block, 0)
        piece_values = lax.dynamic_slice_in_dim(values, offset, block, 0)
        key_pos = offset + jnp.arange(block)
        return (
            combine(state, partial_attention(query, piece_keys, piece_values, mask_of(key_pos))),
            None,
        )

    offsets = jnp.arange(count // block) * block
    state, unused = lax.scan(one_block, carry, offsets)
    return state


def on_device(hidden, w_query, w_key, w_value, prompt_len, page_table):
    local = hidden[0]
    rows = local.shape[0]
    width = w_query.shape[1]
    heads = width // HD
    seq_index = lax.axis_index("seq")
    is_prompt = lax.axis_index("grp") == 0
    empty = jnp.zeros((rows, width), jnp.float32)
    piece = (
        lax.all_gather(w_query, "seq", axis=0, tiled=True),
        lax.all_gather(w_key, "seq", axis=0, tiled=True),
        lax.all_gather(w_value, "seq", axis=0, tiled=True),
    )
    projected = tuple(
        (jnp.dot(local, weight, preferred_element_type=jnp.float32) for weight in piece)
    )
    query, keys, values = [item.astype(jnp.bfloat16) for item in projected]
    positions = seq_index * rows + jnp.arange(rows)
    start_state = (
        jnp.full((heads, rows), NEG, jnp.float32),
        jnp.zeros((heads, rows), jnp.float32),
        empty,
    )
    given_keys, given_values = from_behind((keys, values), "grp", 1)
    cache_keys = jnp.where(is_prompt, keys, given_keys)
    cache_values = jnp.where(is_prompt, values, given_values)
    row_count = rows // STEPS
    own_tables = lax.dynamic_slice_in_dim(page_table, seq_index * row_count, row_count, 0)
    own_lengths = lax.dynamic_slice_in_dim(prompt_len, seq_index * row_count, row_count, 0)

    def mask_of(key_pos):
        causal = key_pos[None, :] <= positions[:, None]
        listed = row_mask(own_tables, own_lengths, key_pos)
        return jnp.where(is_prompt, causal, listed)

    piece = (
        lax.all_gather(cache_keys, "seq", axis=0, tiled=True),
        lax.all_gather(cache_values, "seq", axis=0, tiled=True),
    )
    state = blocked(start_state, piece[0], piece[1], query, mask_of)
    frame_row = positions // STEPS
    own_rows = (frame_row[:, None] == frame_row[None, :]) & (
        positions[None, :] <= positions[:, None]
    )
    fresh = partial_attention(query, keys, values, own_rows)
    prefill_out = finish(state)
    decode_out = finish(combine(state, fresh))
    return jnp.where(is_prompt, prefill_out, decode_out)[None]


QUERY, KEY, VALUE = 0, 1, 2
ORDER = (KEY, VALUE, QUERY)
SUBS = 1
LAG = 1
PARTS = 2


def fused_kernel(
    hidden, w_query, w_key, w_value, lengths_in, tables_in, out,
    lengths, tables, hbuf, near, far, far_q, acc, qbuf, fresh, cache, bias, osend, orecv,
    y_send, y_recv, x_send, x_recv, d_send, d_recv, local_sem,
    kx_send, kx_recv, ky_send, ky_recv, o_send, o_recv,
):
    weights = {QUERY: w_query, KEY: w_key, VALUE: w_value}
    rows = hidden.shape[1]
    depth = w_query.shape[0]
    half = w_query.shape[1] // 2
    heads = half // HD
    chip_rows = 2 * rows
    grp = lax.axis_index("grp")
    seq = lax.axis_index("seq")
    y = seq // 2
    core = seq % 2
    partner = {"seq": 2 * y + 1 - core}
    across = [{"seq": 2 * (1 - y) + core}, {"seq": 2 * (1 - y) + 1 - core}]
    beside = {"grp": 1 - grp}
    core_of = [core, 1 - core]
    piece = depth // 2 // SUBS

    barrier = pltpu.get_barrier_semaphore()
    for other in (partner, across[0], across[1], beside):
        pl.semaphore_signal(barrier, inc=1, device_id=other, device_id_type=pl.DeviceIdType.MESH)
    pl.semaphore_wait(barrier, 4)

    def remote(src, dst, send, recv, to):
        return pltpu.make_async_remote_copy(
            src_ref=src, dst_ref=dst, send_sem=send, recv_sem=recv,
            device_id=to, device_id_type=pl.DeviceIdType.MESH,
        )

    def columns(which):
        return pl.ds(pl.multiple_of(core_of[which] * half, half), half)

    kv_steps = [(m, sub, rel) for m in (KEY, VALUE) for sub in range(SUBS) for rel in range(2)]
    q_steps = [(QUERY, head, rel) for head in range(heads) for rel in range(2)]
    steps = kv_steps + q_steps

    def slot(m, rel, way, sub):
        if m == QUERY:
            return (sub * 2 + rel) * 2 + way
        return (((m - KEY) * SUBS + sub) * 2 + rel) * 2 + way

    def landing(m, rel, way, sub):
        return (far_q if m == QUERY else far).at[slot(m, rel, way, sub)]

    def number(m, rel, way, sub):
        return slot(m, rel, way, sub) + (8 * SUBS if m == QUERY else 0)

    def weight_copy(m, sub, rel):
        if m == QUERY:
            span = pl.ds(pl.multiple_of(grp * (depth // 2), depth // 2), depth // 2)
            across_lanes = pl.ds(pl.multiple_of(core_of[rel] * half + sub * HD, HD), HD)
        else:
            span = pl.ds(pl.multiple_of(grp * (depth // 2) + sub * piece, piece), piece)
            across_lanes = columns(rel)
        at = number(m, rel, 0, sub)
        return remote(
            weights[m].at[span, across_lanes], landing(m, rel, 0, sub),
            y_send.at[at], y_recv.at[at], across[rel],
        )

    def forward_copy(m, sub, rel):
        at = number(m, rel, 1, sub)
        return remote(
            landing(m, rel, 0, sub), landing(m, rel, 1, sub), x_send.at[at], x_recv.at[at], beside
        )

    sent = []
    for step in steps:
        copy = weight_copy(*step)
        copy.start()
        sent.append(copy)
    my_rows = pl.ds(pl.multiple_of(core * rows, rows), rows)
    hidden_swap = remote(hidden.at[0], hbuf.at[my_rows], d_send.at[3], d_recv.at[3], partner)
    hidden_swap.start()
    swaps = {
        m: remote(weights[m].at[:, columns(1)], near.at[2 * m + 1], d_send.at[m], d_recv.at[m], partner)
        for m in ORDER
    }
    keeps = {
        m: pltpu.make_async_copy(weights[m].at[:, columns(0)], near.at[2 * m], local_sem.at[m])
        for m in ORDER
    }
    hidden_keep = pltpu.make_async_copy(hidden.at[0], hbuf.at[my_rows], local_sem.at[3])
    hidden_keep.start()
    for m in ORDER:
        keeps[m].start()
        swaps[m].start()
    sent += [hidden_swap] + [swaps[m] for m in ORDER]

    table_keep = pltpu.make_async_copy(tables_in, tables, local_sem.at[4])
    length_keep = pltpu.make_async_copy(lengths_in, lengths, local_sem.at[5])
    table_keep.start()
    length_keep.start()
    table_keep.wait()
    length_keep.wait()

    decode_rows = chip_rows // STEPS
    pages = 2 * chip_rows // PAGE
    own_rows = pl.ds(pl.multiple_of(y * decode_rows, decode_rows), decode_rows)
    own_table = tables[:, own_rows]
    own_length = lengths[:, own_rows]
    page_row = lax.broadcasted_iota(jnp.int32, (pages, decode_rows), 0)
    member = own_table[0:1, :] == page_row
    for listed in range(1, own_table.shape[0]):
        member = member | (own_table[listed : listed + 1, :] == page_row)
    member = jnp.where(member, 1.0, 0.0).astype(jnp.bfloat16)
    step_bits = STEPS.bit_length() - 1
    page_bits = PAGE.bit_length() - 1
    spread = (
        lax.shift_right_logical(lax.broadcasted_iota(jnp.int32, (chip_rows, decode_rows), 0), step_bits)
        == lax.broadcasted_iota(jnp.int32, (chip_rows, decode_rows), 1)
    )
    spread = jnp.where(spread, 1.0, 0.0).astype(jnp.bfloat16)
    prompt_one = jnp.where(grp == 0, 1, 0)
    contract_last = (((1,), (1,)), ((), ()))
    for side in range(2):
        base = (y if side == 0 else 1 - y) * chip_rows
        key_page = lax.shift_right_logical(
            lax.broadcasted_iota(jnp.int32, (chip_rows, pages), 0) + base, page_bits
        )
        unfold = lax.broadcasted_iota(jnp.int32, (chip_rows, pages), 1) == key_page
        unfold = jnp.where(unfold, 1.0, 0.0).astype(jnp.bfloat16)
        seen = jnp.dot(unfold, member, preferred_element_type=jnp.float32)
        key_pos = lax.broadcasted_iota(jnp.int32, (chip_rows, decode_rows), 0) + base
        seen = jnp.where(key_pos < own_length, seen, 0.0).astype(jnp.bfloat16)
        listed = lax.dot_general(spread, seen, contract_last, preferred_element_type=jnp.float32)
        causal = (
            lax.broadcasted_iota(jnp.int32, (chip_rows, chip_rows), 1) + base
            <= lax.broadcasted_iota(jnp.int32, (chip_rows, chip_rows), 0) + y * chip_rows
        )
        causal = jnp.where(causal, 1.0, 0.0)
        allowed = jnp.where(prompt_one == 1, causal, listed)
        bias[:, side * chip_rows : (side + 1) * chip_rows] = jnp.where(allowed > 0.5, 0.0, NEG)

    def add(m, weight, first, count, fresh_start=False):
        left = hbuf[:, pl.ds(pl.multiple_of(first, count), count)]
        product = jnp.dot(left, weight, preferred_element_type=jnp.float32)
        if fresh_start:
            acc[m] = product
        else:
            acc[m] += product

    hidden_keep.wait()
    hidden_swap.wait_recv()
    for m in ORDER:
        keeps[m].wait()
        add(m, near[2 * m], (2 * y + core) * depth, depth, True)
        swaps[m].wait_recv()
        add(m, near[2 * m + 1], (2 * y + 1 - core) * depth, depth)

    def from_across(m, sub, rel, way):
        owner = grp if way == 0 else 1 - grp
        first = (2 * (1 - y) + core_of[rel]) * depth + owner * (depth // 2)
        weight = landing(m, rel, way, sub)[...]
        if m != QUERY:
            add(m, weight, first + sub * piece, piece)
            return
        left = hbuf[:, pl.ds(pl.multiple_of(first, depth // 2), depth // 2)]
        acc[m, :, sub * HD : (sub + 1) * HD] += jnp.dot(
            left, weight, preferred_element_type=jnp.float32
        )

    def take_y(step):
        weight_copy(*step).wait_recv()
        copy = forward_copy(*step)
        copy.start()
        sent.append(copy)
        from_across(*step, 0)

    def take_x(step):
        forward_copy(*step).wait_recv()
        from_across(*step, 1)

    kv_pieces = [(kind, part) for kind in range(2) for part in range(PARTS)]
    part_rows = chip_rows // PARTS

    def piece_of(ref, at, part):
        return ref.at[at, pl.ds(part * part_rows, part_rows)]

    def kx_copy(kind, part):
        at = kind * PARTS + part
        return remote(
            piece_of(fresh, kind, part), piece_of(cache, kind, part), kx_send.at[at], kx_recv.at[at], beside
        )

    def ky_copy(kind, part, source):
        at = kind * PARTS + part
        return remote(
            piece_of(source, kind, part), piece_of(cache, 2 + kind, part),
            ky_send.at[at], ky_recv.at[at], across[0],
        )

    def settle(kind, m):
        fresh[kind] = acc[m].astype(jnp.bfloat16)

        @pl.when(grp == 0)
        def _():
            for part in range(PARTS):
                kx_copy(kind, part).start()
                ky_copy(kind, part, fresh).start()
            cache[kind] = acc[m].astype(jnp.bfloat16)

    lag = LAG
    settled = {(KEY, SUBS - 1, 1): (0, KEY), (VALUE, SUBS - 1, 1): (1, VALUE)}
    for index in range(len(kv_steps) + lag):
        take_y(steps[index])
        if index >= lag:
            step = steps[index - lag]
            take_x(step)
            if step in settled:
                settle(*settled[step])

    for step in q_steps[lag:]:
        take_y(step)

    @pl.when(grp != 0)
    def _():
        for kind, part in kv_pieces:
            kx_copy(kind, part).wait_recv()
            ky_copy(kind, part, cache).start()

    block = min(rows, 128)
    fresh_row = lax.broadcasted_iota(jnp.int32, (block, block), 0)
    fresh_col = lax.broadcasted_iota(jnp.int32, (block, block), 1)
    same = (
        lax.shift_right_logical(fresh_row, step_bits) == lax.shift_right_logical(fresh_col, step_bits)
    ) & (fresh_col <= fresh_row)
    fresh_bias = jnp.where(jnp.where(same, 1 - prompt_one, 0) == 1, 0.0, NEG)
    scale = HD ** (-0.5)

    def attend(first, head):
        span = pl.ds(pl.multiple_of(first, block), block)
        lanes = slice(head * HD, (head + 1) * HD)
        query = qbuf[span, lanes]

        def scored(keys, mask):
            return lax.dot_general(
                query, keys, contract_last, preferred_element_type=jnp.float32
            ) * scale + mask

        scores = [
            scored(cache[0, :, lanes], bias[span, 0:chip_rows]),
            scored(cache[2, :, lanes], bias[span, chip_rows : 2 * chip_rows]),
            scored(fresh[0, span, lanes], fresh_bias),
        ]
        values = [cache[1, :, lanes], cache[3, :, lanes], fresh[1, span, lanes]]
        top = jnp.maximum(
            jnp.maximum(
                jnp.max(scores[0], axis=1, keepdims=True), jnp.max(scores[1], axis=1, keepdims=True)
            ),
            jnp.max(scores[2], axis=1, keepdims=True),
        )
        total = jnp.zeros((block, 1), jnp.float32)
        summed = jnp.zeros((block, HD), jnp.float32)
        for score, value in zip(scores, values):
            weight = jnp.exp(score - top)
            total += jnp.sum(weight, axis=1, keepdims=True)
            summed += jnp.dot(weight.astype(jnp.bfloat16), value, preferred_element_type=jnp.float32)
        return (summed / total).astype(jnp.bfloat16)

    swaps_out = []
    for head in range(heads):
        lanes = slice(head * HD, (head + 1) * HD)
        for rel in range(2):
            take_x((QUERY, head, rel))
        qbuf[:, lanes] = acc[QUERY, :, lanes].astype(jnp.bfloat16)
        if head == 0:
            for kind, part in kv_pieces:
                ky_copy(kind, part, cache).wait_recv()
        for at in range(rows // block):
            osend[head, at * block : (at + 1) * block] = attend((1 - core) * rows + at * block, head)
        swap_out = remote(osend.at[head], orecv.at[head], o_send.at[head], o_recv.at[head], partner)
        swap_out.start()
        swaps_out.append(swap_out)
        for at in range(rows // block):
            own_lanes = pl.ds(pl.multiple_of(core * half + head * HD, HD), HD)
            out[at * block : (at + 1) * block, own_lanes] = attend(core * rows + at * block, head)
    for head, swap_out in enumerate(swaps_out):
        swap_out.wait()
        out[:, pl.ds(pl.multiple_of((1 - core) * half + head * HD, HD), HD)] = orecv[head]

    for copy in sent:
        copy.wait_send()

    @pl.when(grp == 0)
    def _():
        for kind, part in kv_pieces:
            kx_copy(kind, part).wait_send()
            ky_copy(kind, part, fresh).wait_send()

    @pl.when(grp != 0)
    def _():
        for kind, part in kv_pieces:
            ky_copy(kind, part, cache).wait_send()


def fused(hidden, w_query, w_key, w_value, prompt_len, page_table):
    rows, model = hidden.shape[1:]
    depth, width = w_query.shape
    half = width // 2
    chip_rows = 2 * rows
    heads = half // HD
    copies = 8 * SUBS + 4 * heads
    dma = pltpu.SemaphoreType.DMA
    anywhere = pl.BlockSpec(memory_space=pltpu.HBM)
    vmem = pl.BlockSpec(memory_space=pltpu.VMEM)
    result = pl.pallas_call(
        fused_kernel,
        out_shape=jax.ShapeDtypeStruct((rows, width), jnp.bfloat16),
        in_specs=[anywhere] * 6,
        out_specs=vmem,
        scratch_shapes=[
            pltpu.VMEM((1, prompt_len.shape[0]), jnp.int32),
            pltpu.VMEM(page_table.shape[::-1], jnp.int32),
            pltpu.VMEM((chip_rows, model), jnp.bfloat16),
            pltpu.VMEM((6, depth, half), jnp.bfloat16),
            pltpu.VMEM((8 * SUBS, depth // 2 // SUBS, half), jnp.bfloat16),
            pltpu.VMEM((4 * heads, depth // 2, HD), jnp.bfloat16),
            pltpu.VMEM((3, chip_rows, half), jnp.float32),
            pltpu.VMEM((chip_rows, half), jnp.bfloat16),
            pltpu.VMEM((2, chip_rows, half), jnp.bfloat16),
            pltpu.VMEM((4, chip_rows, half), jnp.bfloat16),
            pltpu.VMEM((chip_rows, 2 * chip_rows), jnp.float32),
            pltpu.VMEM((heads, rows, HD), jnp.bfloat16),
            pltpu.VMEM((heads, rows, HD), jnp.bfloat16),
            dma((copies,)), dma((copies,)), dma((copies,)), dma((copies,)),
            dma((4,)), dma((4,)), dma((6,)),
            dma((2 * PARTS,)), dma((2 * PARTS,)), dma((2 * PARTS,)), dma((2 * PARTS,)),
            dma((heads,)), dma((heads,)),
        ],
        compiler_params=pltpu.CompilerParams(
            collective_id=0, has_side_effects=True, vmem_limit_bytes=67043328
        ),
    )(hidden, w_query, w_key, w_value, prompt_len.reshape(1, -1), page_table.T)
    return result[None]


def solution(mesh):
    paired = mesh.shape["grp"] == 2 and mesh.shape["seq"] == 4
    return jax.shard_map(
        fused if paired else on_device,
        mesh=mesh,
        in_specs=(P("grp", "seq", None), P("seq", "tp"), P("seq", "tp"), P("seq", "tp"), P(), P()),
        out_specs=P("grp", "seq", "tp"),
        check_vma=False,
    )
```
